256 devices in a mesh: rows: 16 (over z, core), wide: 16 (over y, x).
Axes of the slice: x: 4, y: 4, z: 8, core: 2. Of those that a mesh axis runs over, the one named last changes fastest.
Arguments:
- matrix_tiles: bfloat16 [2048, 16, 128, 128], P('rows', 'wide'), may hold values from -1.5 to 1.5
- row_pointers: int32 [272, 16], P('rows', 'wide'), may hold values from 0 to 112, as said below
- column_blocks: int32 [2048, 16], P('rows', 'wide'), may hold values from 0 to 4095, as said below
- prolongator_tiles: bfloat16 [256, 16, 2, 128, 128], P('rows', 'wide'), may hold values from -0.5 to 0.5
- aggregate_ids: int32 [256, 16, 2], P('rows', 'wide'), may hold values from 0 to 1023, as said below
Outputs:
- coarse_band: bfloat16 [64, 16, 36, 128, 128], P('rows', 'wide')
The draws below stay inside these ranges and needn't reach their ends.
Inputs may be any that keep to these rules, and one draw needn't show every extreme that they name: `row_pointers`: each device's pointers start at 0 and rise by at least 1 for each of its 16 row blocks; its last pointer, its count of used slots, is at most 112. For two devices with the same rows index whose wide indices differ by 8 the two counts add up to at most 128; in every draw some such pair adds up to exactly 128 and some device holds exactly 112. `column_blocks`: every slot, used or not, names a fine block of its own device, of one of the 4 fine block rows nearest to it on the device beside it along rows, on a device beside it along wide, or on a device beside it along both; the first slot of each row block names that row block. `aggregate_ids`: each names a coarse block owned by the device that owns the fine block: coarse rows 4 r to 4 r + 3 and the same wide index.
All inputs are finite; a program needn't handle non-finite values.
Results may differ from the reference program's by a relative error of at most 0.005.
Values may be sent and summed in bfloat16 or wider, within the bound.
A program may use at most 128 MiB of HBM per device.

```python
import jax
import jax.numpy as jnp
from jax import lax

TILE = 128
P_TILES = 2
FINE = 16
COARSE = 4
COUPLED_BLOCKS = 4
SLOTS = 128
FINE_ROWS = 256
COARSE_ROWS = 64
N_ROWS = 16
N_WIDE = 16


def slot_layout(key):
    halfway = N_WIDE // 2
    heavy = jax.random.randint(jax.random.fold_in(key, 1), (N_ROWS, halfway), FINE, SLOTS - FINE + 1)
    light = jax.random.randint(jax.random.fold_in(key, 2), (N_ROWS, halfway), FINE, SLOTS - heavy + 1)
    chosen = jax.random.randint(jax.random.fold_in(key, 3), (N_ROWS, 1), 0, halfway)
    pair_index = jnp.arange(halfway, dtype=jnp.int32)[None, :]
    heavy = jnp.where(pair_index == chosen, SLOTS - FINE, heavy)
    light = jnp.where(pair_index == chosen, FINE, light)
    flipped = jax.random.randint(jax.random.fold_in(key, 4), (N_ROWS, halfway), 0, 2) == 1
    lower = jnp.where(flipped, light, heavy)
    upper = jnp.where(flipped, heavy, light)
    counts = jnp.concatenate([lower, upper], axis=1)
    extra_rows = jax.random.randint(jax.random.fold_in(key, 5), (N_ROWS, N_WIDE, SLOTS), 0, FINE)
    used = jnp.arange(SLOTS, dtype=jnp.int32)[None, None, :] < (counts - FINE)[:, :, None]
    matches = (extra_rows[..., None] == jnp.arange(FINE, dtype=jnp.int32)) & used[..., None]
    lengths = 1 + jnp.sum(matches.astype(jnp.int32), axis=2)
    zeros = jnp.zeros((N_ROWS, N_WIDE, 1), jnp.int32)
    return jnp.concatenate([zeros, jnp.cumsum(lengths, axis=-1).astype(jnp.int32)], axis=-1)


def draw_row_pointers(key, part):
    pointers = slot_layout(key)
    return jnp.transpose(pointers, (0, 2, 1)).reshape(N_ROWS * (FINE + 1), N_WIDE)


def pick_shift(key, shape, index, limit):
    code = jax.random.randint(key, shape, 0, 6)
    shift = jnp.where(code == 0, -1, jnp.where(code == 1, 1, 0))
    target = index + shift
    return jnp.where((target >= 0) & (target < limit), shift, 0)


def draw_column_blocks(key, part):
    pointers = slot_layout(key)
    slot_ids = jnp.arange(SLOTS, dtype=jnp.int32)
    below = pointers[:, :, None, 1:] <= slot_ids[None, None, :, None]
    slot_row = jnp.minimum(jnp.sum(below.astype(jnp.int32), axis=-1), FINE - 1)
    start_offsets = jnp.take_along_axis(pointers, slot_row, axis=2)
    leading = slot_ids[None, None, :] == start_offsets
    shape = (N_ROWS, N_WIDE, SLOTS)
    row_index = jnp.arange(N_ROWS, dtype=jnp.int32)[:, None, None]
    wide_index = jnp.arange(N_WIDE, dtype=jnp.int32)[None, :, None]
    row_shift = pick_shift(jax.random.fold_in(key, 6), shape, row_index, N_ROWS)
    wide_shift = pick_shift(jax.random.fold_in(key, 7), shape, wide_index, N_WIDE)
    nearby = jax.random.randint(jax.random.fold_in(key, 8), shape, 0, COUPLED_BLOCKS)
    anywhere = jax.random.randint(jax.random.fold_in(key, 9), shape, 0, FINE)
    local_block = jnp.where(row_shift == -1, FINE - 1 - nearby, jnp.where(row_shift == 1, nearby, anywhere))
    fine_row = (row_index + row_shift) * FINE + local_block
    fine_wide = wide_index + wide_shift
    fine_row = jnp.where(leading, row_index * FINE + slot_row, fine_row)
    fine_wide = jnp.where(leading, wide_index, fine_wide)
    block_ids = (fine_row * N_WIDE + fine_wide).astype(jnp.int32)
    return jnp.transpose(block_ids, (0, 2, 1)).reshape(N_ROWS * SLOTS, N_WIDE)


def draw_aggregate_ids(key, part):
    choice_ids = jax.random.randint(jax.random.fold_in(key, 21), (FINE * N_ROWS, N_WIDE, P_TILES), 0, COARSE)
    fine_row = jnp.arange(FINE * N_ROWS, dtype=jnp.int32)[:, None, None]
    wide_index = jnp.arange(N_WIDE, dtype=jnp.int32)[None, :, None]
    return ((fine_row // FINE * COARSE + choice_ids) * N_WIDE + wide_index).astype(jnp.int32)


def shard_levels(key, dims, cuts, low, largest):
    def one(axis_at, blocks):
        heights = jax.random.uniform(jax.random.fold_in(jax.random.fold_in(key, 6), axis_at), (blocks,), jnp.float32, low / len(cuts), largest / len(cuts))
        return jnp.repeat(jnp.exp(heights), dims[axis_at] // blocks).reshape((-1,) + (1,) * (len(dims) - axis_at - 1))

    factor_of = one(*cuts[0])
    for cut in cuts[1:]:
        factor_of = factor_of * one(*cut)
    return factor_of


def centred(stream_key, extent, deviation, most, split=(), kind=jnp.bfloat16):
    values = jax.random.normal(stream_key, extent, jnp.float32) * deviation
    if len(split) > 0:
        values = shard_levels(stream_key, extent, split, -0.22, 0.18) * values
    return jnp.clip(values, min=-most, max=most).astype(kind)


def setup_inputs(seed: int = 0) -> dict:
    seeds = jax.random.split(jax.random.key(seed), 6)
    return {
        "matrix_tiles": centred(seeds[0], (SLOTS * N_ROWS, N_WIDE, TILE, TILE), 16 ** -0.5, 1.5, ((0, 16), (1, 16))),
        "row_pointers": draw_row_pointers(jax.random.fold_in(seeds[5], 71), 0),
        "column_blocks": draw_column_blocks(jax.random.fold_in(seeds[5], 71), 0),
        "prolongator_tiles": centred(seeds[3], (FINE_ROWS, N_WIDE, P_TILES, TILE, TILE), TILE ** -0.5, 0.5, ((0, 16), (1, 16))),
        "aggregate_ids": draw_aggregate_ids(jax.random.fold_in(seeds[5], 71), 0),
    }


def reference(matrix_tiles, row_pointers, column_blocks, prolongator_tiles, aggregate_ids):
    tile_grid = matrix_tiles.reshape(N_ROWS, SLOTS, N_WIDE, TILE, TILE)
    pointers = row_pointers.reshape(N_ROWS, FINE + 1, N_WIDE)
    columns = column_blocks.reshape(N_ROWS, SLOTS, N_WIDE)
    band_size = 9 * COARSE
    row_index = jnp.arange(N_ROWS, dtype=jnp.int32)[:, None]
    wide_index = jnp.arange(N_WIDE, dtype=jnp.int32)[None, :]
    result = jnp.zeros((COARSE_ROWS, N_WIDE, band_size, TILE, TILE), jnp.float32)

    def add_slot(slot, result):
        slot = jnp.asarray(slot).astype(jnp.int32)
        operator = lax.dynamic_index_in_dim(tile_grid, slot, 1, keepdims=False)
        column = lax.dynamic_index_in_dim(columns, slot, 1, keepdims=False).astype(jnp.int32)
        active = slot < pointers[:, FINE, :]
        block_row = jnp.sum((pointers[:, 1:, :] <= slot).astype(jnp.int32), axis=1)
        block_row = jnp.minimum(block_row, FINE - 1)
        fine_row = (row_index * FINE + block_row).astype(jnp.int32)
        fine_wide = jnp.broadcast_to(wide_index, fine_row.shape).astype(jnp.int32)
        near_row = (column // N_WIDE).astype(jnp.int32)
        near_wide = (column % N_WIDE).astype(jnp.int32)
        own_p = prolongator_tiles[fine_row, fine_wide].astype(jnp.float32)
        far_p = prolongator_tiles[near_row, near_wide].astype(jnp.float32)
        product = jnp.einsum('rwab,rwmbc->rwmac', operator.astype(jnp.float32), far_p,
                             precision=lax.Precision.HIGHEST).astype(jnp.bfloat16)
        term_tiles = jnp.einsum('rwnba,rwmbc->rwnmac', own_p, product.astype(jnp.float32),
                                precision=lax.Precision.HIGHEST)
        term_tiles = jnp.where(active[:, :, None, None, None, None], term_tiles, jnp.float32(0.0))
        first_ids = aggregate_ids[fine_row, fine_wide]
        second_ids = aggregate_ids[near_row, near_wide]
        first_row = first_ids // N_WIDE
        first_wide = first_ids % N_WIDE
        second_row = second_ids // N_WIDE
        second_wide = second_ids % N_WIDE
        offset = ((second_row[:, :, None, :] // COARSE - first_row[:, :, :, None] // COARSE + 1) * 3
                  + (second_wide[:, :, None, :] - first_wide[:, :, :, None] + 1)) * COARSE \
            + second_row[:, :, None, :] % COARSE
        shape = offset.shape
        target_row = jnp.broadcast_to(first_row[:, :, :, None], shape).astype(jnp.int32)
        target_wide = jnp.broadcast_to(first_wide[:, :, :, None], shape).astype(jnp.int32)
        return result.at[target_row, target_wide, offset.astype(jnp.int32)].add(term_tiles)

    result = lax.fori_loop(0, SLOTS, add_slot, result)
    return result.astype(jnp.bfloat16)
```

```python
import functools

import jax
import jax.numpy as jnp
from jax import lax
from jax.experimental import pallas as pl
from jax.experimental.pallas import tpu as pltpu
from jax.sharding import PartitionSpec as P

TILE = 128
P_TILES = 2
FINE = 16
COARSE = 4
HALO = 4
SLOTS = 128
LIVE = 112
SPAN = FINE + 2 * HALO
WIDE_M = COARSE * TILE
CHUNK_ORDER = (0, 3, 1, 2)
MESH = pl.DeviceIdType.MESH
ROWS_M, ROWS_P = 0, 1


def exact_log2(n):
    bits = n.bit_length() - 1
    assert 1 << bits == n
    return bits


def kernel(
    n_rows,
    n_wide,
    ptr_ref,
    ids_ref,
    col_ref,
    a_hbm,
    p_hbm,
    out_ref,
    a_v,
    ext,
    ext_id,
    own_t,
    r_v,
    phat,
    acc,
    racc,
    meta_v,
    meta_s,
    load_sem,
    meta_sem,
    wide_send,
    wide_recv,
    wid_send,
    wid_recv,
    halo_send,
    halo_recv,
    hid_send,
    hid_recv,
):
    f32, bf16, i32 = jnp.float32, jnp.bfloat16, jnp.int32
    r = lax.axis_index("rows")
    w = lax.axis_index("wide")
    row_peer = (lax.rem(r + n_rows - 1, n_rows), lax.rem(r + 1, n_rows))
    wide_peer = (lax.rem(w + n_wide - 1, n_wide), lax.rem(w + 1, n_wide))
    wide_bits = exact_log2(n_wide)

    barrier = pltpu.get_barrier_semaphore()
    for peer in row_peer:
        pl.semaphore_signal(barrier, inc=1, device_id=(peer, w), device_id_type=MESH)
    for peer in wide_peer:
        pl.semaphore_signal(barrier, inc=1, device_id=(r, peer), device_id_type=MESH)

    loads = []
    own_load = pltpu.make_async_copy(p_hbm.at[:, 0], ext.at[1, pl.ds(HALO, FINE)], load_sem.at[0])
    own_load.start()
    for q in range(4):
        part = pl.ds(q * (LIVE // 4), LIVE // 4)
        load = pltpu.make_async_copy(a_hbm.at[part, 0], a_v.at[part], load_sem.at[1 + q])
        load.start()
        loads.append(load)

    for i in range(FINE):
        for m in range(P_TILES):
            local = lax.shift_right_logical(ids_ref[m, i], wide_bits) & (COARSE - 1)
            ext_id[1, pl.ds((HALO + i) * P_TILES + m, 1), :] = jnp.full((1, TILE), local, i32).astype(f32)

    pl.semaphore_wait(barrier, 4)

    def to_wide(d, chunk):
        side = 0 if d == 1 else 2
        return pltpu.make_async_remote_copy(
            src_ref=p_hbm.at[pl.ds(chunk * HALO, HALO), 0],
            dst_ref=ext.at[side, pl.ds(HALO + chunk * HALO, HALO)],
            send_sem=wide_send.at[d, chunk],
            recv_sem=wide_recv.at[d, chunk],
            device_id=(r, wide_peer[d]),
            device_id_type=MESH,
        )

    def to_wide_id(d):
        side = 0 if d == 1 else 2
        part = pl.ds(HALO * P_TILES, FINE * P_TILES)
        return pltpu.make_async_remote_copy(
            src_ref=ext_id.at[1, part],
            dst_ref=ext_id.at[side, part],
            send_sem=wid_send.at[d],
            recv_sem=wid_recv.at[d],
            device_id=(r, wide_peer[d]),
            device_id_type=MESH,
        )

    def to_rows(d, side):
        source = FINE if d == 1 else HALO
        target = 0 if d == 1 else HALO + FINE
        if side == 1:
            src = p_hbm.at[pl.ds(source - HALO, HALO), 0]
        else:
            src = ext.at[side, pl.ds(source, HALO)]
        return pltpu.make_async_remote_copy(
            src_ref=src,
            dst_ref=ext.at[side, pl.ds(target, HALO)],
            send_sem=halo_send.at[d, side],
            recv_sem=halo_recv.at[d, side],
            device_id=(row_peer[d], w),
            device_id_type=MESH,
        )

    def to_rows_id(d, side):
        source = FINE if d == 1 else HALO
        target = 0 if d == 1 else HALO + FINE
        return pltpu.make_async_remote_copy(
            src_ref=ext_id.at[side, pl.ds(source * P_TILES, HALO * P_TILES)],
            dst_ref=ext_id.at[side, pl.ds(target * P_TILES, HALO * P_TILES)],
            send_sem=hid_send.at[d, side],
            recv_sem=hid_recv.at[d, side],
            device_id=(row_peer[d], w),
            device_id_type=MESH,
        )

    for chunk in CHUNK_ORDER:
        for d in (0, 1):
            to_wide(d, chunk).start()
        if chunk == 0:
            for d in (0, 1):
                to_rows(d, 1).start()

    lane = lax.broadcasted_iota(i32, (TILE, SLOTS), 1)
    sub = lax.broadcasted_iota(i32, (TILE, SLOTS), 0)
    col = jnp.broadcast_to(col_ref[...], (TILE, SLOTS))
    near_row = lax.shift_right_logical(col, wide_bits) - r * FINE + HALO
    near_wide = (col & (n_wide - 1)) - w + 1
    key_l = jnp.where(lane < ptr_ref[FINE], near_wide * SPAN + near_row, 3 * SPAN)
    row_l = jnp.zeros((TILE, SLOTS), i32)
    for k in range(1, FINE):
        row_l = row_l + (lane >= ptr_ref[k]).astype(i32)
    key_s = key_l.T
    row_s = row_l.T
    same = key_s == key_l
    ahead = (key_s < key_l) | (same & (sub < lane))
    rank_l = jnp.sum(ahead.astype(i32), axis=0, keepdims=True)
    later_l = jnp.sum((same & (sub < lane)).astype(i32), axis=0, keepdims=True)
    rank_s = jnp.broadcast_to(rank_l, (TILE, SLOTS)).T
    later_s = jnp.broadcast_to(later_l, (TILE, SLOTS)).T
    chosen = rank_s == lane

    def pick(values):
        return jnp.sum(jnp.where(chosen, values, 0), axis=0, keepdims=True)

    upto = jnp.sum((key_s <= lane).astype(i32), axis=0, keepdims=True)
    count = jnp.sum((key_s == lane).astype(i32), axis=0, keepdims=True)
    meta_v[0:1, :] = pick(sub)
    meta_v[1:2, :] = pick(row_s)
    meta_v[2:3, :] = pick((later_s > 0).astype(i32))
    meta_v[3:4, :] = jnp.where(count > 0, upto - 1, LIVE)
    meta_v[4:8, :] = jnp.zeros((4, TILE), i32)
    r_v[LIVE] = jnp.zeros((WIDE_M, TILE), bf16)
    racc[...] = jnp.zeros((WIDE_M, TILE), f32)

    own_load.wait()

    def id_mask(side, index, c):
        return (ext_id[side, pl.ds(index, 1), :] == jnp.float32(c)).astype(f32).astype(bf16)

    for d in (0, 1):
        to_wide_id(d).start()
        to_rows_id(d, 1).start()

    @pl.loop(0, FINE)
    def _(i):
        first = ext[1, HALO + i, 0].T
        second = ext[1, HALO + i, 1].T
        for c in range(COARSE):
            own_t[i, c * TILE : (c + 1) * TILE, :] = first * id_mask(1, (HALO + i) * P_TILES, c) + second * id_mask(
                1, (HALO + i) * P_TILES + 1, c
            )

    meta_copy = pltpu.make_async_copy(meta_v, meta_s, meta_sem)
    meta_copy.start()
    meta_copy.wait()
    for load in loads:
        load.wait()

    @pl.loop(0, LIVE)
    def _(k):
        tile = a_v[jnp.clip(meta_s[0, k], 0, LIVE - 1)]
        left = own_t[jnp.clip(meta_s[1, k], 0, FINE - 1)]
        keep = meta_s[2, k].astype(f32)
        total = racc[...] * keep + jnp.dot(left, tile, preferred_element_type=f32)
        racc[...] = total
        r_v[k] = total.astype(bf16)

    def chunk_product(side, row, slot):
        for l in range(HALO):
            index = (row + l) * P_TILES
            first = ext[side, row + l, 0]
            second = ext[side, row + l, 1]
            for c in range(COARSE):
                phat[slot, l * TILE : (l + 1) * TILE, c * TILE : (c + 1) * TILE] = first * id_mask(
                    side, index, c
                ) + second * id_mask(side, index + 1, c)
        base = side * SPAN + row
        left = jnp.concatenate([r_v[jnp.clip(meta_s[3, base + l], 0, LIVE)] for l in range(HALO)], axis=1)
        return jnp.dot(left, phat[slot], preferred_element_type=f32)

    def put(code, value):
        for c1 in range(COARSE):
            for c2 in range(COARSE):
                out_ref[c1, 0, code * COARSE + c2] = value[
                    c1 * TILE : (c1 + 1) * TILE, c2 * TILE : (c2 + 1) * TILE
                ].astype(bf16)

    acc[1] = chunk_product(1, HALO, 0)

    @pl.loop(1, FINE // HALO - 1)
    def _(q):
        acc[1] += chunk_product(1, HALO + q * HALO, 0)

    put(4, acc[1] + chunk_product(1, FINE, 1))

    for d in (0, 1):
        to_wide_id(d).wait_recv()
        to_wide(d, 0).wait_recv()
        to_rows(0, 0 if d == 1 else 2).start()
        to_rows_id(0, 0 if d == 1 else 2).start()
    for d in (0, 1):
        side = 0 if d == 1 else 2
        acc[side] = chunk_product(side, HALO, d)
    for d in (0, 1):
        to_wide(d, 3).wait_recv()
        to_rows(1, 0 if d == 1 else 2).start()
        to_rows_id(1, 0 if d == 1 else 2).start()
    for d in (0, 1):
        side = 0 if d == 1 else 2
        acc[side] += chunk_product(side, FINE, d)

    for d in (0, 1):
        to_rows(d, 1).wait_recv()
        to_rows_id(d, 1).wait_recv()
        step = 0 if d == 1 else 2
        put(step * 3 + 1, chunk_product(1, 0 if d == 1 else HALO + FINE, d))

    for d in (0, 1):
        side = 0 if d == 1 else 2
        to_wide(d, 1).wait_recv()
        acc[side] += chunk_product(side, 2 * HALO, d)

    for d in (0, 1):
        for side in (0, 2):
            to_rows(d, side).wait_recv()
            to_rows_id(d, side).wait_recv()
            step = 0 if d == 1 else 2
            put(step * 3 + side, chunk_product(side, 0 if d == 1 else HALO + FINE, side // 2))

    for d in (0, 1):
        side = 0 if d == 1 else 2
        to_wide(d, 2).wait_recv()
        put(3 + side, acc[side] + chunk_product(side, 3 * HALO, d))

    for d in (0, 1):
        to_wide_id(d).wait_send()
        for chunk in CHUNK_ORDER:
            to_wide(d, chunk).wait_send()
        for side in (0, 1, 2):
            to_rows(d, side).wait_send()
            to_rows_id(d, side).wait_send()


def body(matrix_tiles, row_pointers, column_blocks, prolongator_tiles, aggregate_ids):
    n_rows, n_wide = lax.axis_size("rows"), lax.axis_size("wide")
    bf16, f32, i32 = jnp.bfloat16, jnp.float32, jnp.int32
    dma = pltpu.SemaphoreType.DMA
    smem = pl.BlockSpec(memory_space=pltpu.SMEM)
    anywhere = pl.BlockSpec(memory_space=pl.ANY)
    vmem = pl.BlockSpec(memory_space=pltpu.VMEM)
    return pl.pallas_call(
        functools.partial(kernel, n_rows, n_wide),
        out_shape=jax.ShapeDtypeStruct((COARSE, 1, 9 * COARSE, TILE, TILE), bf16),
        in_specs=[smem, smem, vmem, anywhere, anywhere],
        out_specs=vmem,
        scratch_shapes=[
            pltpu.VMEM((LIVE, TILE, TILE), bf16),
            pltpu.VMEM((3, SPAN, P_TILES, TILE, TILE), bf16),
            pltpu.VMEM((3, SPAN * P_TILES, TILE), f32),
            pltpu.VMEM((FINE, WIDE_M, TILE), bf16),
            pltpu.VMEM((LIVE + 1, WIDE_M, TILE), bf16),
            pltpu.VMEM((2, HALO * TILE, WIDE_M), bf16),
            pltpu.VMEM((3, WIDE_M, WIDE_M), f32),
            pltpu.VMEM((WIDE_M, TILE), f32),
            pltpu.VMEM((8, TILE), i32),
            pltpu.SMEM((8, TILE), i32),
            dma((5,)),
            dma,
            dma((2, 4)),
            dma((2, 4)),
            dma((2,)),
            dma((2,)),
            dma((2, 3)),
            dma((2, 3)),
            dma((2, 3)),
            dma((2, 3)),
        ],
        compiler_params=pltpu.CompilerParams(
            collective_id=0, has_side_effects=True, vmem_limit_bytes=56 * 1024 * 1024
        ),
        name="galerkin",
    )(
        row_pointers.reshape(FINE + 1),
        aggregate_ids.transpose(1, 2, 0).reshape(P_TILES, FINE),
        column_blocks.reshape(1, SLOTS),
        matrix_tiles,
        prolongator_tiles,
    )


def solution(mesh):
    placed = (
        P("rows", "wide", None, None),
        P("rows", "wide"),
        P("rows", "wide"),
        P("rows", "wide", None, None, None),
        P("rows", "wide", None),
    )
    return jax.shard_map(
        body,
        mesh=mesh,
        in_specs=placed,
        out_specs=P("rows", "wide", None, None, None),
        check_vma=False,
    )
```

```python
import functools

import jax
import jax.numpy as jnp
from jax import lax
from jax.experimental import pallas as pl
from jax.experimental.pallas import tpu as pltpu
from jax.sharding import PartitionSpec as P

TILE = 128
P_TILES = 2
FINE = 16
COARSE = 4
HALO = 4
SLOTS = 128
LIVE = 112
SPAN = FINE + 2 * HALO
WIDE_M = COARSE * TILE
CHUNK_ORDER = (0, 3, 1, 2)
MESH = pl.DeviceIdType.MESH
ROWS_M, ROWS_P = 0, 1


def exact_log2(n):
    bits = n.bit_length() - 1
    assert 1 << bits == n
    return bits


def kernel(
    n_rows,
    n_wide,
    ptr_ref,
    ids_ref,
    col_ref,
    a_hbm,
    p_hbm,
    out_ref,
    a_v,
    ext,
    ext_id,
    own_t,
    r_v,
    phat,
    acc,
    racc,
    meta_v,
    meta_s,
    load_sem,
    meta_sem,
    wide_send,
    wide_recv,
    wid_send,
    wid_recv,
    halo_send,
    halo_recv,
    hid_send,
    hid_recv,
):
    f32, bf16, i32 = jnp.float32, jnp.bfloat16, jnp.int32
    r = lax.axis_index("rows")
    w = lax.axis_index("wide")
    row_peer = (lax.rem(r + n_rows - 1, n_rows), lax.rem(r + 1, n_rows))
    wide_peer = (lax.rem(w + n_wide - 1, n_wide), lax.rem(w + 1, n_wide))
    wide_bits = exact_log2(n_wide)

    barrier = pltpu.get_barrier_semaphore()
    for peer in row_peer:
        pl.semaphore_signal(barrier, inc=1, device_id=(peer, w), device_id_type=MESH)
    for peer in wide_peer:
        pl.semaphore_signal(barrier, inc=1, device_id=(r, peer), device_id_type=MESH)

    loads = []
    own_load = pltpu.make_async_copy(p_hbm.at[:, 0], ext.at[1, pl.ds(HALO, FINE)], load_sem.at[0])
    own_load.start()
    for q in range(4):
        part = pl.ds(q * (LIVE // 4), LIVE // 4)
        load = pltpu.make_async_copy(a_hbm.at[part, 0], a_v.at[part], load_sem.at[1 + q])
        load.start()
        loads.append(load)

    for i in range(FINE):
        for m in range(P_TILES):
            local = lax.shift_right_logical(ids_ref[m, i], wide_bits) & (COARSE - 1)
            ext_id[1, pl.ds((HALO + i) * P_TILES + m, 1), :] = jnp.full((1, TILE), local, i32).astype(f32)

    pl.semaphore_wait(barrier, 4)

    def to_wide(d, chunk):
        side = 0 if d == 1 else 2
        return pltpu.make_async_remote_copy(
            src_ref=p_hbm.at[pl.ds(chunk * HALO, HALO), 0],
            dst_ref=ext.at[side, pl.ds(HALO + chunk * HALO, HALO)],
            send_sem=wide_send.at[d, chunk],
            recv_sem=wide_recv.at[d, chunk],
            device_id=(r, wide_peer[d]),
            device_id_type=MESH,
        )

    def to_wide_id(d):
        side = 0 if d == 1 else 2
        part = pl.ds(HALO * P_TILES, FINE * P_TILES)
        return pltpu.make_async_remote_copy(
            src_ref=ext_id.at[1, part],
            dst_ref=ext_id.at[side, part],
            send_sem=wid_send.at[d],
            recv_sem=wid_recv.at[d],
            device_id=(r, wide_peer[d]),
            device_id_type=MESH,
        )

    def to_rows(d, side):
        source = FINE if d == 1 else HALO
        target = 0 if d == 1 else HALO + FINE
        if side == 1:
            src = p_hbm.at[pl.ds(source - HALO, HALO), 0]
        else:
            src = ext.at[side, pl.ds(source, HALO)]
        return pltpu.make_async_remote_copy(
            src_ref=src,
            dst_ref=ext.at[side, pl.ds(target, HALO)],
            send_sem=halo_send.at[d, side],
            recv_sem=halo_recv.at[d, side],
            device_id=(row_peer[d], w),
            device_id_type=MESH,
        )

    def to_rows_id(d, side):
        source = FINE if d == 1 else HALO
        target = 0 if d == 1 else HALO + FINE
        return pltpu.make_async_remote_copy(
            src_ref=ext_id.at[side, pl.ds(source * P_TILES, HALO * P_TILES)],
            dst_ref=ext_id.at[side, pl.ds(target * P_TILES, HALO * P_TILES)],
            send_sem=hid_send.at[d, side],
            recv_sem=hid_recv.at[d, side],
            device_id=(row_peer[d], w),
            device_id_type=MESH,
        )

    for chunk in CHUNK_ORDER:
        for d in (0, 1):
            to_wide(d, chunk).start()
        if chunk == 0:
            for d in (0, 1):
                to_wide_id(d).start()
                to_rows_id(d, 1).start()
                to_rows(d, 1).start()

    lane = lax.broadcasted_iota(i32, (TILE, SLOTS), 1)
    sub = lax.broadcasted_iota(i32, (TILE, SLOTS), 0)
    col = jnp.broadcast_to(col_ref[...], (TILE, SLOTS))
    near_row = lax.shift_right_logical(col, wide_bits) - r * FINE + HALO
    near_wide = (col & (n_wide - 1)) - w + 1
    key_l = jnp.where(lane < ptr_ref[FINE], near_wide * SPAN + near_row, 3 * SPAN)
    row_l = jnp.zeros((TILE, SLOTS), i32)
    for k in range(1, FINE):
        row_l = row_l + (lane >= ptr_ref[k]).astype(i32)
    key_s = key_l.T
    row_s = row_l.T
    same = key_s == key_l
    ahead = (key_s < key_l) | (same & (sub < lane))
    rank_l = jnp.sum(ahead.astype(i32), axis=0, keepdims=True)
    later_l = jnp.sum((same & (sub < lane)).astype(i32), axis=0, keepdims=True)
    rank_s = jnp.broadcast_to(rank_l, (TILE, SLOTS)).T
    later_s = jnp.broadcast_to(later_l, (TILE, SLOTS)).T
    chosen = rank_s == lane

    def pick(values):
        return jnp.sum(jnp.where(chosen, values, 0), axis=0, keepdims=True)

    upto = jnp.sum((key_s <= lane).astype(i32), axis=0, keepdims=True)
    count = jnp.sum((key_s == lane).astype(i32), axis=0, keepdims=True)
    meta_v[0:1, :] = pick(sub)
    meta_v[1:2, :] = pick(row_s)
    meta_v[2:3, :] = pick((later_s > 0).astype(i32))
    meta_v[3:4, :] = jnp.where(count > 0, upto - 1, LIVE)
    meta_v[4:8, :] = jnp.zeros((4, TILE), i32)
    r_v[LIVE] = jnp.zeros((WIDE_M, TILE), bf16)
    racc[...] = jnp.zeros((WIDE_M, TILE), f32)

    own_load.wait()

    def id_mask(side, index, c):
        return (ext_id[side, pl.ds(index, 1), :] == jnp.float32(c)).astype(f32).astype(bf16)

    @pl.loop(0, FINE)
    def _(i):
        first = ext[1, HALO + i, 0].T
        second = ext[1, HALO + i, 1].T
        for c in range(COARSE):
            own_t[i, c * TILE : (c + 1) * TILE, :] = first * id_mask(1, (HALO + i) * P_TILES, c) + second * id_mask(
                1, (HALO + i) * P_TILES + 1, c
            )

    meta_copy = pltpu.make_async_copy(meta_v, meta_s, meta_sem)
    meta_copy.start()
    meta_copy.wait()
    for load in loads:
        load.wait()

    @pl.loop(0, LIVE, unroll=8)
    def _(k):
        tile = a_v[jnp.clip(meta_s[0, k], 0, LIVE - 1)]
        left = own_t[jnp.clip(meta_s[1, k], 0, FINE - 1)]
        keep = meta_s[2, k].astype(f32)
        total = racc[...] * keep + jnp.dot(left, tile, preferred_element_type=f32)
        racc[...] = total
        r_v[k] = total.astype(bf16)

    def chunk_product(side, row, slot):
        for l in range(HALO):
            index = (row + l) * P_TILES
            first = ext[side, row + l, 0]
            second = ext[side, row + l, 1]
            for c in range(COARSE):
                phat[slot, l * TILE : (l + 1) * TILE, c * TILE : (c + 1) * TILE] = first * id_mask(
                    side, index, c
                ) + second * id_mask(side, index + 1, c)
        base = side * SPAN + row
        left = jnp.concatenate([r_v[jnp.clip(meta_s[3, base + l], 0, LIVE)] for l in range(HALO)], axis=1)
        return jnp.dot(left, phat[slot], preferred_element_type=f32)

    def put(code, value):
        for c1 in range(COARSE):
            for c2 in range(COARSE):
                out_ref[c1, 0, code * COARSE + c2] = value[
                    c1 * TILE : (c1 + 1) * TILE, c2 * TILE : (c2 + 1) * TILE
                ].astype(bf16)

    acc[1] = chunk_product(1, HALO, 0)

    @pl.loop(1, FINE // HALO - 1)
    def _(q):
        acc[1] += chunk_product(1, HALO + q * HALO, 0)

    put(4, acc[1] + chunk_product(1, FINE, 1))

    for d in (0, 1):
        to_wide_id(d).wait_recv()
        to_wide(d, 0).wait_recv()
        to_rows(0, 0 if d == 1 else 2).start()
        to_rows_id(0, 0 if d == 1 else 2).start()
    for d in (0, 1):
        side = 0 if d == 1 else 2
        acc[side] = chunk_product(side, HALO, d)
    for d in (0, 1):
        to_wide(d, 3).wait_recv()
        to_rows(1, 0 if d == 1 else 2).start()
        to_rows_id(1, 0 if d == 1 else 2).start()
    for d in (0, 1):
        side = 0 if d == 1 else 2
        acc[side] += chunk_product(side, FINE, d)

    for d in (0, 1):
        to_rows(d, 1).wait_recv()
        to_rows_id(d, 1).wait_recv()
        step = 0 if d == 1 else 2
        put(step * 3 + 1, chunk_product(1, 0 if d == 1 else HALO + FINE, d))

    for d in (0, 1):
        side = 0 if d == 1 else 2
        to_wide(d, 1).wait_recv()
        acc[side] += chunk_product(side, 2 * HALO, d)

    for d in (0, 1):
        for side in (0, 2):
            to_rows(d, side).wait_recv()
            to_rows_id(d, side).wait_recv()
            step = 0 if d == 1 else 2
            put(step * 3 + side, chunk_product(side, 0 if d == 1 else HALO + FINE, side // 2))

    for d in (0, 1):
        side = 0 if d == 1 else 2
        to_wide(d, 2).wait_recv()
        put(3 + side, acc[side] + chunk_product(side, 3 * HALO, d))

    for d in (0, 1):
        to_wide_id(d).wait_send()
        for chunk in CHUNK_ORDER:
            to_wide(d, chunk).wait_send()
        for side in (0, 1, 2):
            to_rows(d, side).wait_send()
            to_rows_id(d, side).wait_send()


def body(matrix_tiles, row_pointers, column_blocks, prolongator_tiles, aggregate_ids):
    n_rows, n_wide = lax.axis_size("rows"), lax.axis_size("wide")
    bf16, f32, i32 = jnp.bfloat16, jnp.float32, jnp.int32
    dma = pltpu.SemaphoreType.DMA
    smem = pl.BlockSpec(memory_space=pltpu.SMEM)
    anywhere = pl.BlockSpec(memory_space=pltpu.HBM)
    vmem = pl.BlockSpec(memory_space=pltpu.VMEM)
    return pl.pallas_call(
        functools.partial(kernel, n_rows, n_wide),
        out_shape=pltpu.VMEM((COARSE, 1, 9 * COARSE, TILE, TILE), bf16),
        in_specs=[smem, smem, vmem, anywhere, anywhere],
        out_specs=vmem,
        scratch_shapes=[
            pltpu.VMEM((LIVE, TILE, TILE), bf16),
            pltpu.VMEM((3, SPAN, P_TILES, TILE, TILE), bf16),
            pltpu.VMEM((3, SPAN * P_TILES, TILE), f32),
            pltpu.VMEM((FINE, WIDE_M, TILE), bf16),
            pltpu.VMEM((LIVE + 1, WIDE_M, TILE), bf16),
            pltpu.VMEM((2, HALO * TILE, WIDE_M), bf16),
            pltpu.VMEM((3, WIDE_M, WIDE_M), f32),
            pltpu.VMEM((WIDE_M, TILE), f32),
            pltpu.VMEM((8, TILE), i32),
            pltpu.SMEM((8, TILE), i32),
            dma((5,)),
            dma,
            dma((2, 4)),
            dma((2, 4)),
            dma((2,)),
            dma((2,)),
            dma((2, 3)),
            dma((2, 3)),
            dma((2, 3)),
            dma((2, 3)),
        ],
        compiler_params=pltpu.CompilerParams(
            collective_id=0, has_side_effects=True, vmem_limit_bytes=57344 * 1024
        ),
        name="galerkin",
    )(
        row_pointers.reshape(FINE + 1),
        aggregate_ids.transpose(1, 2, 0).reshape(P_TILES, FINE),
        column_blocks.reshape(1, SLOTS),
        matrix_tiles,
        prolongator_tiles,
    )


def solution(mesh):
    placed = (
        P("rows", "wide", None, None),
        P("rows", "wide"),
        P("rows", "wide"),
        P("rows", "wide", None, None, None),
        P("rows", "wide", None),
    )
    return jax.shard_map(
        body,
        mesh=mesh,
        in_specs=placed,
        out_specs=P("rows", "wide", None, None, None),
        check_vma=False,
    )
```

```python
import functools

import jax
import jax.numpy as jnp
from jax import lax
from jax.experimental import pallas as pl
from jax.experimental.pallas import tpu as pltpu
from jax.sharding import PartitionSpec as P

TILE = 128
P_TILES = 2
FINE = 16
COARSE = 4
HALO = 4
SLOTS = 128
LIVE = 112
SPAN = FINE + 2 * HALO
WIDE_M = COARSE * TILE
PIECES = ((0, 4), (12, 4), (4, 4), (8, 2), (10, 2))
MESH = pl.DeviceIdType.MESH


def exact_log2(n):
    bits = n.bit_length() - 1
    assert 1 << bits == n
    return bits


def kernel(
    n_rows,
    n_wide,
    ptr_ref,
    ids_ref,
    col_ref,
    a_hbm,
    p_hbm,
    out_ref,
    a_v,
    ext,
    ext_id,
    own_t,
    r_v,
    phat,
    acc,
    racc,
    meta_v,
    meta_s,
    load_sem,
    meta_sem,
    wide_send,
    wide_recv,
    wid_send,
    wid_recv,
    halo_send,
    halo_recv,
    hid_send,
    hid_recv,
):
    f32, bf16, i32 = jnp.float32, jnp.bfloat16, jnp.int32
    r = lax.axis_index("rows")
    w = lax.axis_index("wide")
    row_peer, has_row = (r - 1, r + 1), (r > 0, r < n_rows - 1)
    wide_peer, has_wide = (w - 1, w + 1), (w > 0, w < n_wide - 1)
    has_side = {0: has_wide[0], 2: has_wide[1]}
    wide_bits = exact_log2(n_wide)

    barrier = pltpu.get_barrier_semaphore()
    for d in (0, 1):

        @pl.when(has_wide[d])
        def _():
            pl.semaphore_signal(barrier, inc=1, device_id=(r, wide_peer[d]), device_id_type=MESH)

        @pl.when(has_row[d])
        def _():
            pl.semaphore_signal(barrier, inc=1, device_id=(row_peer[d], w), device_id_type=MESH)

    loads = []
    own_load = pltpu.make_async_copy(p_hbm.at[:, 0], ext.at[1, pl.ds(HALO, FINE)], load_sem.at[0])
    own_load.start()
    for q in range(4):
        part = pl.ds(q * (LIVE // 4), LIVE // 4)
        load = pltpu.make_async_copy(a_hbm.at[part, 0], a_v.at[part], load_sem.at[1 + q])
        load.start()
        loads.append(load)

    for i in range(FINE):
        for m in range(P_TILES):
            local = lax.shift_right_logical(ids_ref[m, i], wide_bits) & (COARSE - 1)
            ext_id[1, pl.ds((HALO + i) * P_TILES + m, 1), :] = jnp.full((1, TILE), local, i32).astype(f32)

    for d in (0, 1):
        side = 2 * d

        @pl.when(jnp.logical_not(has_wide[d]))
        def _():
            ext_id[side] = jnp.zeros((SPAN * P_TILES, TILE), f32)

            @pl.loop(0, SPAN)
            def _(i):
                ext[side, i] = jnp.zeros((P_TILES, TILE, TILE), bf16)

        @pl.when(jnp.logical_not(has_row[d]))
        def _():
            row = d * (HALO + FINE)
            for side in (0, 1, 2):
                ext_id[side, pl.ds(row * P_TILES, HALO * P_TILES), :] = jnp.zeros((HALO * P_TILES, TILE), f32)

                @pl.loop(0, HALO)
                def _(i):
                    ext[side, row + i] = jnp.zeros((P_TILES, TILE, TILE), bf16)

    pl.semaphore_wait(barrier, sum(there.astype(i32) for there in has_row + has_wide))

    def to_wide(d, piece):
        side = 0 if d == 1 else 2
        row, rows = PIECES[piece]
        return pltpu.make_async_remote_copy(
            src_ref=p_hbm.at[pl.ds(row, rows), 0],
            dst_ref=ext.at[side, pl.ds(HALO + row, rows)],
            send_sem=wide_send.at[d, piece],
            recv_sem=wide_recv.at[d, piece],
            device_id=(r, wide_peer[d]),
            device_id_type=MESH,
        )

    def to_wide_id(d):
        side = 0 if d == 1 else 2
        part = pl.ds(HALO * P_TILES, FINE * P_TILES)
        return pltpu.make_async_remote_copy(
            src_ref=ext_id.at[1, part],
            dst_ref=ext_id.at[side, part],
            send_sem=wid_send.at[d],
            recv_sem=wid_recv.at[d],
            device_id=(r, wide_peer[d]),
            device_id_type=MESH,
        )

    def to_rows(d, side):
        source = FINE if d == 1 else HALO
        target = 0 if d == 1 else HALO + FINE
        if side == 1:
            src = p_hbm.at[pl.ds(source - HALO, HALO), 0]
        else:
            src = ext.at[side, pl.ds(source, HALO)]
        return pltpu.make_async_remote_copy(
            src_ref=src,
            dst_ref=ext.at[side, pl.ds(target, HALO)],
            send_sem=halo_send.at[d, side],
            recv_sem=halo_recv.at[d, side],
            device_id=(row_peer[d], w),
            device_id_type=MESH,
        )

    def to_rows_id(d, side):
        source = FINE if d == 1 else HALO
        target = 0 if d == 1 else HALO + FINE
        return pltpu.make_async_remote_copy(
            src_ref=ext_id.at[side, pl.ds(source * P_TILES, HALO * P_TILES)],
            dst_ref=ext_id.at[side, pl.ds(target * P_TILES, HALO * P_TILES)],
            send_sem=hid_send.at[d, side],
            recv_sem=hid_recv.at[d, side],
            device_id=(row_peer[d], w),
            device_id_type=MESH,
        )

    for d in (0, 1):

        @pl.when(has_wide[d])
        def _():
            to_wide(d, 0).start()
            to_wide_id(d).start()

    for d in (0, 1):

        @pl.when(has_row[d])
        def _():
            to_rows_id(d, 1).start()
            to_rows(d, 1).start()

    for d in (0, 1):

        @pl.when(has_wide[d])
        def _():
            for piece in range(1, len(PIECES)):
                to_wide(d, piece).start()

    lane = lax.broadcasted_iota(i32, (TILE, SLOTS), 1)
    sub = lax.broadcasted_iota(i32, (TILE, SLOTS), 0)
    col = jnp.broadcast_to(col_ref[...], (TILE, SLOTS))
    near_row = lax.shift_right_logical(col, wide_bits) - r * FINE + HALO
    near_wide = (col & (n_wide - 1)) - w + 1
    key_l = jnp.where(lane < ptr_ref[FINE], near_wide * SPAN + near_row, 3 * SPAN)
    row_l = jnp.zeros((TILE, SLOTS), i32)
    for k in range(1, FINE):
        row_l = row_l + (lane >= ptr_ref[k]).astype(i32)
    key_s = key_l.T
    row_s = row_l.T
    same = key_s == key_l
    ahead = (key_s < key_l) | (same & (sub < lane))
    rank_l = jnp.sum(ahead.astype(i32), axis=0, keepdims=True)
    later_l = jnp.sum((same & (sub < lane)).astype(i32), axis=0, keepdims=True)
    rank_s = jnp.broadcast_to(rank_l, (TILE, SLOTS)).T
    later_s = jnp.broadcast_to(later_l, (TILE, SLOTS)).T
    chosen = rank_s == lane

    def pick(values):
        return jnp.sum(jnp.where(chosen, values, 0), axis=0, keepdims=True)

    upto = jnp.sum((key_s <= lane).astype(i32), axis=0, keepdims=True)
    count = jnp.sum((key_s == lane).astype(i32), axis=0, keepdims=True)
    meta_v[0:1, :] = pick(sub)
    meta_v[1:2, :] = pick(row_s)
    meta_v[2:3, :] = pick((later_s > 0).astype(i32))
    meta_v[3:4, :] = jnp.where(count > 0, upto - 1, LIVE)
    meta_v[4:8, :] = jnp.zeros((4, TILE), i32)
    r_v[LIVE] = jnp.zeros((WIDE_M, TILE), bf16)
    racc[...] = jnp.zeros((WIDE_M, TILE), f32)

    own_load.wait()

    def id_mask(side, index, c):
        return (ext_id[side, pl.ds(index, 1), :] == jnp.float32(c)).astype(f32).astype(bf16)

    @pl.loop(0, FINE)
    def _(i):
        first = ext[1, HALO + i, 0].T
        second = ext[1, HALO + i, 1].T
        for c in range(COARSE):
            own_t[i, c * TILE : (c + 1) * TILE, :] = first * id_mask(1, (HALO + i) * P_TILES, c) + second * id_mask(
                1, (HALO + i) * P_TILES + 1, c
            )

    meta_copy = pltpu.make_async_copy(meta_v, meta_s, meta_sem)
    meta_copy.start()
    meta_copy.wait()
    for load in loads:
        load.wait()

    @pl.loop(0, LIVE, unroll=8)
    def _(k):
        tile = a_v[jnp.clip(meta_s[0, k], 0, LIVE - 1)]
        left = own_t[jnp.clip(meta_s[1, k], 0, FINE - 1)]
        keep = meta_s[2, k].astype(f32)
        total = racc[...] * keep + jnp.dot(left, tile, preferred_element_type=f32)
        racc[...] = total
        r_v[k] = total.astype(bf16)

    def chunk_product(side, row, slot, rows=HALO):
        for l in range(rows):
            index = (row + l) * P_TILES
            first = ext[side, row + l, 0]
            second = ext[side, row + l, 1]
            for c in range(COARSE):
                phat[slot, l * TILE : (l + 1) * TILE, c * TILE : (c + 1) * TILE] = first * id_mask(
                    side, index, c
                ) + second * id_mask(side, index + 1, c)
        base = side * SPAN + row
        left = jnp.concatenate([r_v[jnp.clip(meta_s[3, base + l], 0, LIVE)] for l in range(rows)], axis=1)
        return jnp.dot(left, phat[slot, : rows * TILE, :], preferred_element_type=f32)

    def put(code, value):
        for c1 in range(COARSE):
            for c2 in range(COARSE):
                out_ref[c1, 0, code * COARSE + c2] = value[
                    c1 * TILE : (c1 + 1) * TILE, c2 * TILE : (c2 + 1) * TILE
                ].astype(bf16)

    acc[1] = chunk_product(1, HALO, 0)

    @pl.loop(1, FINE // HALO - 1)
    def _(q):
        acc[1] += chunk_product(1, HALO + q * HALO, 0)

    put(4, acc[1] + chunk_product(1, FINE, 1))

    for step in (0, 1):
        for d in (0, 1):
            side = 0 if d == 1 else 2

            @pl.when(has_side[side])
            def _():
                if step == 0:
                    to_wide_id(d).wait_recv()
                to_wide(d, step).wait_recv()

                @pl.when(has_row[step])
                def _():
                    to_rows_id(step, side).start()
                    to_rows(step, side).start()

        for d in (0, 1):
            side = 0 if d == 1 else 2
            value = chunk_product(side, HALO + PIECES[step][0], d)
            if step == 0:
                acc[side] = value
            else:
                acc[side] += value

    for d in (0, 1):

        @pl.when(has_row[1 - d])
        def _():
            to_rows(d, 1).wait_recv()
            to_rows_id(d, 1).wait_recv()

        step = 0 if d == 1 else 2
        put(step * 3 + 1, chunk_product(1, 0 if d == 1 else HALO + FINE, d))

    for d in (0, 1):
        side = 0 if d == 1 else 2

        @pl.when(has_side[side])
        def _():
            to_wide(d, 2).wait_recv()

        acc[side] += chunk_product(side, HALO + PIECES[2][0], d)

    for d in (0, 1):
        for side in (0, 2):

            @pl.when(has_row[1 - d] & has_side[side])
            def _():
                to_rows(d, side).wait_recv()
                to_rows_id(d, side).wait_recv()

            step = 0 if d == 1 else 2
            put(step * 3 + side, chunk_product(side, 0 if d == 1 else HALO + FINE, side // 2))

    for d in (0, 1):
        side = 0 if d == 1 else 2

        @pl.when(has_side[side])
        def _():
            to_wide(d, 3).wait_recv()

        acc[side] += chunk_product(side, HALO + PIECES[3][0], d, PIECES[3][1])

    for d in (0, 1):
        side = 0 if d == 1 else 2

        @pl.when(has_side[side])
        def _():
            to_wide(d, 4).wait_recv()

        put(3 + side, acc[side] + chunk_product(side, HALO + PIECES[4][0], d, PIECES[4][1]))

    for d in (0, 1):

        @pl.when(has_wide[d])
        def _():
            to_wide_id(d).wait_send()
            for piece in range(len(PIECES)):
                to_wide(d, piece).wait_send()

        @pl.when(has_row[d])
        def _():
            to_rows(d, 1).wait_send()
            to_rows_id(d, 1).wait_send()

        for side in (0, 2):

            @pl.when(has_row[d] & has_side[side])
            def _():
                to_rows(d, side).wait_send()
                to_rows_id(d, side).wait_send()


def body(matrix_tiles, row_pointers, column_blocks, prolongator_tiles, aggregate_ids):
    n_rows, n_wide = lax.axis_size("rows"), lax.axis_size("wide")
    bf16, f32, i32 = jnp.bfloat16, jnp.float32, jnp.int32
    dma = pltpu.SemaphoreType.DMA
    smem = pl.BlockSpec(memory_space=pltpu.SMEM)
    anywhere = pl.BlockSpec(memory_space=pltpu.HBM)
    vmem = pl.BlockSpec(memory_space=pltpu.VMEM)
    return pl.pallas_call(
        functools.partial(kernel, n_rows, n_wide),
        out_shape=pltpu.VMEM((COARSE, 1, 9 * COARSE, TILE, TILE), bf16),
        in_specs=[smem, smem, vmem, anywhere, anywhere],
        out_specs=vmem,
        scratch_shapes=[
            pltpu.VMEM((LIVE, TILE, TILE), bf16),
            pltpu.VMEM((3, SPAN, P_TILES, TILE, TILE), bf16),
            pltpu.VMEM((3, SPAN * P_TILES, TILE), f32),
            pltpu.VMEM((FINE, WIDE_M, TILE), bf16),
            pltpu.VMEM((LIVE + 1, WIDE_M, TILE), bf16),
            pltpu.VMEM((2, HALO * TILE, WIDE_M), bf16),
            pltpu.VMEM((3, WIDE_M, WIDE_M), f32),
            pltpu.VMEM((WIDE_M, TILE), f32),
            pltpu.VMEM((8, TILE), i32),
            pltpu.SMEM((8, TILE), i32),
            dma((5,)),
            dma,
            dma((2, len(PIECES))),
            dma((2, len(PIECES))),
            dma((2,)),
            dma((2,)),
            dma((2, 3)),
            dma((2, 3)),
            dma((2, 3)),
            dma((2, 3)),
        ],
        compiler_params=pltpu.CompilerParams(
            collective_id=0, has_side_effects=True, vmem_limit_bytes=57344 * 1024
        ),
        name="galerkin",
    )(
        row_pointers.reshape(FINE + 1),
        aggregate_ids.transpose(1, 2, 0).reshape(P_TILES, FINE),
        column_blocks.reshape(1, SLOTS),
        matrix_tiles,
        prolongator_tiles,
    )


def solution(mesh):
    placed = (
        P("rows", "wide", None, None),
        P("rows", "wide"),
        P("rows", "wide"),
        P("rows", "wide", None, None, None),
        P("rows", "wide", None),
    )
    return jax.shard_map(
        body,
        mesh=mesh,
        in_specs=placed,
        out_specs=P("rows", "wide", None, None, None),
        check_vma=False,
    )
```

```python
import functools

import jax
import jax.numpy as jnp
from jax import lax
from jax.experimental import pallas as pl
from jax.experimental.pallas import tpu as pltpu
from jax.sharding import PartitionSpec as P

TILE = 128
P_TILES = 2
FINE = 16
COARSE = 4
HALO = 4
SLOTS = 128
LIVE = 112
SPAN = FINE + 2 * HALO
WIDE_M = COARSE * TILE
PIECES = ((0, 4), (12, 4), (4, 4), (8, 2), (10, 2))
MESH = pl.DeviceIdType.MESH


def exact_log2(n):
    bits = n.bit_length() - 1
    assert 1 << bits == n
    return bits


def kernel(
    n_rows,
    n_wide,
    ptr_ref,
    ids_ref,
    col_ref,
    a_hbm,
    p_hbm,
    out_ref,
    a_v,
    ext,
    ext_id,
    ids_v,
    own_t,
    r_v,
    phat,
    acc,
    racc,
    meta_v,
    meta_s,
    load_sem,
    meta_sem,
    wide_send,
    wide_recv,
    wid_send,
    wid_recv,
    halo_send,
    halo_recv,
    hid_send,
    hid_recv,
):
    f32, bf16, i32 = jnp.float32, jnp.bfloat16, jnp.int32
    r = lax.axis_index("rows")
    w = lax.axis_index("wide")
    row_peer, has_row = (r - 1, r + 1), (r > 0, r < n_rows - 1)
    wide_peer, has_wide = (w - 1, w + 1), (w > 0, w < n_wide - 1)
    has_side = {0: has_wide[0], 2: has_wide[1]}
    wide_bits = exact_log2(n_wide)

    barrier = pltpu.get_barrier_semaphore()
    for d in (0, 1):

        @pl.when(has_wide[d])
        def _():
            pl.semaphore_signal(barrier, inc=1, device_id=(r, wide_peer[d]), device_id_type=MESH)

        @pl.when(has_row[d])
        def _():
            pl.semaphore_signal(barrier, inc=1, device_id=(row_peer[d], w), device_id_type=MESH)

    loads = []
    own_load = pltpu.make_async_copy(p_hbm.at[:, 0], ext.at[1, pl.ds(HALO, FINE)], load_sem.at[0])
    own_load.start()
    for q in range(4):
        part = pl.ds(q * (LIVE // 4), LIVE // 4)
        load = pltpu.make_async_copy(a_hbm.at[part, 0], a_v.at[part], load_sem.at[1 + q])
        load.start()
        loads.append(load)

    id_lane = lax.broadcasted_iota(i32, (8, TILE), 1)
    id_tile = jnp.zeros((8, TILE), i32)
    for i in range(FINE):
        for m in range(P_TILES):
            local = lax.shift_right_logical(ids_ref[m, i], wide_bits) & (COARSE - 1)
            ext_id[1, pl.ds((HALO + i) * P_TILES + m, 1), :] = jnp.full((1, TILE), local, i32).astype(f32)
            id_tile = jnp.where(id_lane == i * P_TILES + m, local, id_tile)
    ids_v[1, 1] = id_tile.astype(f32)

    for d in (0, 1):
        side = 2 * d

        @pl.when(jnp.logical_not(has_wide[d]))
        def _():
            ext_id[side] = jnp.zeros((SPAN * P_TILES, TILE), f32)

            @pl.loop(0, SPAN)
            def _(i):
                ext[side, i] = jnp.zeros((P_TILES, TILE, TILE), bf16)

        @pl.when(jnp.logical_not(has_row[d]))
        def _():
            row = d * (HALO + FINE)
            for side in (0, 1, 2):
                ext_id[side, pl.ds(row * P_TILES, HALO * P_TILES), :] = jnp.zeros((HALO * P_TILES, TILE), f32)

                @pl.loop(0, HALO)
                def _(i):
                    ext[side, row + i] = jnp.zeros((P_TILES, TILE, TILE), bf16)

    own_load.wait()
    pl.semaphore_wait(barrier, sum(there.astype(i32) for there in has_row + has_wide))

    def to_wide(d, piece):
        side = 0 if d == 1 else 2
        row, rows = PIECES[piece]
        return pltpu.make_async_remote_copy(
            src_ref=ext.at[1, pl.ds(HALO + row, rows)],
            dst_ref=ext.at[side, pl.ds(HALO + row, rows)],
            send_sem=wide_send.at[d, piece],
            recv_sem=wide_recv.at[d, piece],
            device_id=(r, wide_peer[d]),
            device_id_type=MESH,
        )

    def to_wide_id(d):
        side = 0 if d == 1 else 2
        return pltpu.make_async_remote_copy(
            src_ref=ids_v.at[1, 1],
            dst_ref=ids_v.at[side, 1],
            send_sem=wid_send.at[d],
            recv_sem=wid_recv.at[d],
            device_id=(r, wide_peer[d]),
            device_id_type=MESH,
        )

    def to_rows(d, side):
        source = FINE if d == 1 else HALO
        target = 0 if d == 1 else HALO + FINE
        return pltpu.make_async_remote_copy(
            src_ref=ext.at[side, pl.ds(source, HALO)],
            dst_ref=ext.at[side, pl.ds(target, HALO)],
            send_sem=halo_send.at[d, side],
            recv_sem=halo_recv.at[d, side],
            device_id=(row_peer[d], w),
            device_id_type=MESH,
        )

    def to_rows_id(d, side):
        return pltpu.make_async_remote_copy(
            src_ref=ids_v.at[side, 1],
            dst_ref=ids_v.at[side, 0 if d == 1 else 2],
            send_sem=hid_send.at[d, side],
            recv_sem=hid_recv.at[d, side],
            device_id=(row_peer[d], w),
            device_id_type=MESH,
        )

    for d in (0, 1):

        @pl.when(has_wide[d])
        def _():
            to_wide(d, 0).start()
            to_wide_id(d).start()

    for d in (0, 1):

        @pl.when(has_row[d])
        def _():
            to_rows_id(d, 1).start()
            to_rows(d, 1).start()

    for d in (0, 1):

        @pl.when(has_wide[d])
        def _():
            for piece in range(1, len(PIECES)):
                to_wide(d, piece).start()

    lane = lax.broadcasted_iota(i32, (TILE, SLOTS), 1)
    sub = lax.broadcasted_iota(i32, (TILE, SLOTS), 0)
    col = jnp.broadcast_to(col_ref[...], (TILE, SLOTS))
    near_row = lax.shift_right_logical(col, wide_bits) - r * FINE + HALO
    near_wide = (col & (n_wide - 1)) - w + 1
    key_l = jnp.where(lane < ptr_ref[FINE], near_wide * SPAN + near_row, 3 * SPAN)
    row_l = jnp.zeros((TILE, SLOTS), i32)
    for k in range(1, FINE):
        row_l = row_l + (lane >= ptr_ref[k]).astype(i32)
    key_s = key_l.T
    row_s = row_l.T
    same = key_s == key_l
    ahead = (key_s < key_l) | (same & (sub < lane))
    rank_l = jnp.sum(ahead.astype(i32), axis=0, keepdims=True)
    later_l = jnp.sum((same & (sub < lane)).astype(i32), axis=0, keepdims=True)
    rank_s = jnp.broadcast_to(rank_l, (TILE, SLOTS)).T
    later_s = jnp.broadcast_to(later_l, (TILE, SLOTS)).T
    chosen = rank_s == lane

    def pick(values):
        return jnp.sum(jnp.where(chosen, values, 0), axis=0, keepdims=True)

    upto = jnp.sum((key_s <= lane).astype(i32), axis=0, keepdims=True)
    count = jnp.sum((key_s == lane).astype(i32), axis=0, keepdims=True)
    meta_v[0:1, :] = pick(sub)
    meta_v[1:2, :] = pick(row_s)
    meta_v[2:3, :] = pick((later_s > 0).astype(i32))
    meta_v[3:4, :] = jnp.where(count > 0, upto - 1, LIVE)
    meta_v[4:8, :] = jnp.zeros((4, TILE), i32)
    r_v[LIVE] = jnp.zeros((WIDE_M, TILE), bf16)
    racc[...] = jnp.zeros((WIDE_M, TILE), f32)

    def spread_ids(side, part):
        table = jnp.broadcast_to(ids_v[side, part, 0:1, :], (TILE, TILE)).T
        first, count, row = ((FINE - HALO, HALO, 0), (0, FINE, HALO), (0, HALO, HALO + FINE))[part]
        ext_id[side, pl.ds(row * P_TILES, count * P_TILES), :] = table[first * P_TILES : (first + count) * P_TILES]

    def id_mask(side, index, c):
        return (ext_id[side, pl.ds(index, 1), :] == jnp.float32(c)).astype(f32).astype(bf16)

    @pl.loop(0, FINE)
    def _(i):
        first = ext[1, HALO + i, 0].T
        second = ext[1, HALO + i, 1].T
        for c in range(COARSE):
            own_t[i, c * TILE : (c + 1) * TILE, :] = first * id_mask(1, (HALO + i) * P_TILES, c) + second * id_mask(
                1, (HALO + i) * P_TILES + 1, c
            )

    meta_copy = pltpu.make_async_copy(meta_v, meta_s, meta_sem)
    meta_copy.start()
    meta_copy.wait()
    for load in loads:
        load.wait()

    @pl.loop(0, LIVE, unroll=8)
    def _(k):
        tile = a_v[jnp.clip(meta_s[0, k], 0, LIVE - 1)]
        left = own_t[jnp.clip(meta_s[1, k], 0, FINE - 1)]
        keep = meta_s[2, k].astype(f32)
        total = racc[...] * keep + jnp.dot(left, tile, preferred_element_type=f32)
        racc[...] = total
        r_v[k] = total.astype(bf16)

    def chunk_product(side, row, slot, rows=HALO):
        for l in range(rows):
            index = (row + l) * P_TILES
            first = ext[side, row + l, 0]
            second = ext[side, row + l, 1]
            for c in range(COARSE):
                phat[slot, l * TILE : (l + 1) * TILE, c * TILE : (c + 1) * TILE] = first * id_mask(
                    side, index, c
                ) + second * id_mask(side, index + 1, c)
        base = side * SPAN + row
        left = jnp.concatenate([r_v[jnp.clip(meta_s[3, base + l], 0, LIVE)] for l in range(rows)], axis=1)
        return jnp.dot(left, phat[slot, : rows * TILE, :], preferred_element_type=f32)

    def put(code, value):
        for c1 in range(COARSE):
            for c2 in range(COARSE):
                out_ref[c1, 0, code * COARSE + c2] = value[
                    c1 * TILE : (c1 + 1) * TILE, c2 * TILE : (c2 + 1) * TILE
                ].astype(bf16)

    acc[1] = chunk_product(1, HALO, 0)

    @pl.loop(1, FINE // HALO - 1)
    def _(q):
        acc[1] += chunk_product(1, HALO + q * HALO, 0)

    put(4, acc[1] + chunk_product(1, FINE, 1))

    for step in (0, 1):
        for d in (0, 1):
            side = 0 if d == 1 else 2

            @pl.when(has_side[side])
            def _():
                if step == 0:
                    to_wide_id(d).wait_recv()
                    spread_ids(side, 1)
                to_wide(d, step).wait_recv()

                @pl.when(has_row[step])
                def _():
                    to_rows_id(step, side).start()
                    to_rows(step, side).start()

        for d in (0, 1):
            side = 0 if d == 1 else 2
            value = chunk_product(side, HALO + PIECES[step][0], d)
            if step == 0:
                acc[side] = value
            else:
                acc[side] += value

    for d in (0, 1):

        @pl.when(has_row[1 - d])
        def _():
            to_rows(d, 1).wait_recv()
            to_rows_id(d, 1).wait_recv()
            spread_ids(1, 0 if d == 1 else 2)

        step = 0 if d == 1 else 2
        put(step * 3 + 1, chunk_product(1, 0 if d == 1 else HALO + FINE, d))

    for d in (0, 1):
        side = 0 if d == 1 else 2

        @pl.when(has_side[side])
        def _():
            to_wide(d, 2).wait_recv()

        acc[side] += chunk_product(side, HALO + PIECES[2][0], d)

    for d in (0, 1):
        for side in (0, 2):

            @pl.when(has_row[1 - d] & has_side[side])
            def _():
                to_rows(d, side).wait_recv()
                to_rows_id(d, side).wait_recv()
                spread_ids(side, 0 if d == 1 else 2)

            step = 0 if d == 1 else 2
            put(step * 3 + side, chunk_product(side, 0 if d == 1 else HALO + FINE, side // 2))

    for d in (0, 1):
        side = 0 if d == 1 else 2

        @pl.when(has_side[side])
        def _():
            to_wide(d, 3).wait_recv()

        acc[side] += chunk_product(side, HALO + PIECES[3][0], d, PIECES[3][1])

    for d in (0, 1):
        side = 0 if d == 1 else 2

        @pl.when(has_side[side])
        def _():
            to_wide(d, 4).wait_recv()

        put(3 + side, acc[side] + chunk_product(side, HALO + PIECES[4][0], d, PIECES[4][1]))

    for d in (0, 1):

        @pl.when(has_wide[d])
        def _():
            to_wide_id(d).wait_send()
            for piece in range(len(PIECES)):
                to_wide(d, piece).wait_send()

        @pl.when(has_row[d])
        def _():
            to_rows(d, 1).wait_send()
            to_rows_id(d, 1).wait_send()

        for side in (0, 2):

            @pl.when(has_row[d] & has_side[side])
            def _():
                to_rows(d, side).wait_send()
                to_rows_id(d, side).wait_send()


def body(matrix_tiles, row_pointers, column_blocks, prolongator_tiles, aggregate_ids):
    n_rows, n_wide = lax.axis_size("rows"), lax.axis_size("wide")
    bf16, f32, i32 = jnp.bfloat16, jnp.float32, jnp.int32
    dma = pltpu.SemaphoreType.DMA
    smem = pl.BlockSpec(memory_space=pltpu.SMEM)
    anywhere = pl.BlockSpec(memory_space=pltpu.HBM)
    vmem = pl.BlockSpec(memory_space=pltpu.VMEM)
    return pl.pallas_call(
        functools.partial(kernel, n_rows, n_wide),
        out_shape=pltpu.VMEM((COARSE, 1, 9 * COARSE, TILE, TILE), bf16),
        in_specs=[smem, smem, vmem, anywhere, anywhere],
        out_specs=vmem,
        scratch_shapes=[
            pltpu.VMEM((LIVE, TILE, TILE), bf16),
            pltpu.VMEM((3, SPAN, P_TILES, TILE, TILE), bf16),
            pltpu.VMEM((3, SPAN * P_TILES, TILE), f32),
            pltpu.VMEM((3, 3, 8, TILE), f32),
            pltpu.VMEM((FINE, WIDE_M, TILE), bf16),
            pltpu.VMEM((LIVE + 1, WIDE_M, TILE), bf16),
            pltpu.VMEM((2, HALO * TILE, WIDE_M), bf16),
            pltpu.VMEM((3, WIDE_M, WIDE_M), f32),
            pltpu.VMEM((WIDE_M, TILE), f32),
            pltpu.VMEM((8, TILE), i32),
            pltpu.SMEM((8, TILE), i32),
            dma((5,)),
            dma,
            dma((2, len(PIECES))),
            dma((2, len(PIECES))),
            dma((2,)),
            dma((2,)),
            dma((2, 3)),
            dma((2, 3)),
            dma((2, 3)),
            dma((2, 3)),
        ],
        compiler_params=pltpu.CompilerParams(
            collective_id=0, has_side_effects=True, vmem_limit_bytes=57344 * 1024
        ),
        name="galerkin",
    )(
        row_pointers.reshape(FINE + 1),
        aggregate_ids.transpose(1, 2, 0).reshape(P_TILES, FINE),
        column_blocks.reshape(1, SLOTS),
        matrix_tiles,
        prolongator_tiles,
    )


def solution(mesh):
    placed = (
        P("rows", "wide", None, None),
        P("rows", "wide"),
        P("rows", "wide"),
        P("rows", "wide", None, None, None),
        P("rows", "wide", None),
    )
    return jax.shard_map(
        body,
        mesh=mesh,
        in_specs=placed,
        out_specs=P("rows", "wide", None, None, None),
        check_vma=False,
    )
```

```python
import functools

import jax
import jax.numpy as jnp
from jax import lax
from jax.experimental import pallas as pl
from jax.experimental.pallas import tpu as pltpu
from jax.sharding import PartitionSpec as P

TILE = 128
P_TILES = 2
FINE = 16
COARSE = 4
HALO = 4
SLOTS = 128
LIVE = 112
SPAN = FINE + 2 * HALO
WIDE_M = COARSE * TILE
PIECES = ((0, 4), (12, 4), (4, 4), (8, 3), (11, 1))
MESH = pl.DeviceIdType.MESH


def exact_log2(n):
    bits = n.bit_length() - 1
    assert 1 << bits == n
    return bits


def kernel(
    n_rows,
    n_wide,
    ptr_ref,
    ids_ref,
    col_ref,
    a_hbm,
    p_hbm,
    out_ref,
    a_v,
    ext,
    ext_id,
    ids_v,
    own_t,
    r_v,
    phat,
    acc,
    racc,
    meta_v,
    meta_s,
    load_sem,
    meta_sem,
    wide_send,
    wide_recv,
    wid_send,
    wid_recv,
    halo_send,
    halo_recv,
    hid_send,
    hid_recv,
):
    f32, bf16, i32 = jnp.float32, jnp.bfloat16, jnp.int32
    r = lax.axis_index("rows")
    w = lax.axis_index("wide")
    row_peer, has_row = (r - 1, r + 1), (r > 0, r < n_rows - 1)
    wide_peer, has_wide = (w - 1, w + 1), (w > 0, w < n_wide - 1)
    has_side = {0: has_wide[0], 2: has_wide[1]}
    wide_bits = exact_log2(n_wide)

    barrier = pltpu.get_barrier_semaphore()
    for d in (0, 1):

        @pl.when(has_wide[d])
        def _():
            pl.semaphore_signal(barrier, inc=1, device_id=(r, wide_peer[d]), device_id_type=MESH)

        @pl.when(has_row[d])
        def _():
            pl.semaphore_signal(barrier, inc=1, device_id=(row_peer[d], w), device_id_type=MESH)

    loads = []
    own_load = pltpu.make_async_copy(p_hbm.at[:, 0], ext.at[1, pl.ds(HALO, FINE)], load_sem.at[0])
    own_load.start()
    for q in range(4):
        part = pl.ds(q * (LIVE // 4), LIVE // 4)
        load = pltpu.make_async_copy(a_hbm.at[part, 0], a_v.at[part], load_sem.at[1 + q])
        load.start()
        loads.append(load)

    id_lane = lax.broadcasted_iota(i32, (8, TILE), 1)
    id_tile = jnp.zeros((8, TILE), i32)
    for i in range(FINE):
        for m in range(P_TILES):
            local = lax.shift_right_logical(ids_ref[m, i], wide_bits) & (COARSE - 1)
            ext_id[1, pl.ds((HALO + i) * P_TILES + m, 1), :] = jnp.full((1, TILE), local, i32).astype(f32)
            id_tile = jnp.where(id_lane == i * P_TILES + m, local, id_tile)
    ids_v[1, 1] = id_tile.astype(f32)

    for d in (0, 1):
        side = 2 * d

        @pl.when(jnp.logical_not(has_wide[d]))
        def _():
            ext_id[side] = jnp.zeros((SPAN * P_TILES, TILE), f32)

            @pl.loop(0, SPAN)
            def _(i):
                ext[side, i] = jnp.zeros((P_TILES, TILE, TILE), bf16)

        @pl.when(jnp.logical_not(has_row[d]))
        def _():
            row = d * (HALO + FINE)
            for side in (0, 1, 2):
                ext_id[side, pl.ds(row * P_TILES, HALO * P_TILES), :] = jnp.zeros((HALO * P_TILES, TILE), f32)

                @pl.loop(0, HALO)
                def _(i):
                    ext[side, row + i] = jnp.zeros((P_TILES, TILE, TILE), bf16)

    own_load.wait()
    pl.semaphore_wait(barrier, sum(there.astype(i32) for there in has_row + has_wide))

    def to_wide(d, piece):
        side = 0 if d == 1 else 2
        row, rows = PIECES[piece]
        return pltpu.make_async_remote_copy(
            src_ref=ext.at[1, pl.ds(HALO + row, rows)],
            dst_ref=ext.at[side, pl.ds(HALO + row, rows)],
            send_sem=wide_send.at[d, piece],
            recv_sem=wide_recv.at[d, piece],
            device_id=(r, wide_peer[d]),
            device_id_type=MESH,
        )

    def to_wide_id(d):
        side = 0 if d == 1 else 2
        return pltpu.make_async_remote_copy(
            src_ref=ids_v.at[1, 1],
            dst_ref=ids_v.at[side, 1],
            send_sem=wid_send.at[d],
            recv_sem=wid_recv.at[d],
            device_id=(r, wide_peer[d]),
            device_id_type=MESH,
        )

    def to_rows(d, side):
        source = FINE if d == 1 else HALO
        target = 0 if d == 1 else HALO + FINE
        return pltpu.make_async_remote_copy(
            src_ref=ext.at[side, pl.ds(source, HALO)],
            dst_ref=ext.at[side, pl.ds(target, HALO)],
            send_sem=halo_send.at[d, side],
            recv_sem=halo_recv.at[d, side],
            device_id=(row_peer[d], w),
            device_id_type=MESH,
        )

    def to_rows_id(d, side):
        return pltpu.make_async_remote_copy(
            src_ref=ids_v.at[side, 1],
            dst_ref=ids_v.at[side, 0 if d == 1 else 2],
            send_sem=hid_send.at[d, side],
            recv_sem=hid_recv.at[d, side],
            device_id=(row_peer[d], w),
            device_id_type=MESH,
        )

    for d in (0, 1):

        @pl.when(has_wide[d])
        def _():
            to_wide(d, 0).start()
            to_wide_id(d).start()

    for d in (0, 1):

        @pl.when(has_row[d])
        def _():
            to_rows_id(d, 1).start()
            to_rows(d, 1).start()

    for d in (0, 1):

        @pl.when(has_wide[d])
        def _():
            for piece in range(1, len(PIECES)):
                to_wide(d, piece).start()

    lane = lax.broadcasted_iota(i32, (TILE, SLOTS), 1)
    sub = lax.broadcasted_iota(i32, (TILE, SLOTS), 0)
    col = jnp.broadcast_to(col_ref[...], (TILE, SLOTS))
    near_row = lax.shift_right_logical(col, wide_bits) - r * FINE + HALO
    near_wide = (col & (n_wide - 1)) - w + 1
    key_l = jnp.where(lane < ptr_ref[FINE], near_wide * SPAN + near_row, 3 * SPAN)
    row_l = jnp.zeros((TILE, SLOTS), i32)
    for k in range(1, FINE):
        row_l = row_l + (lane >= ptr_ref[k]).astype(i32)
    key_s = key_l.T
    row_s = row_l.T
    same = key_s == key_l
    ahead = (key_s < key_l) | (same & (sub < lane))
    rank_l = jnp.sum(ahead.astype(i32), axis=0, keepdims=True)
    later_l = jnp.sum((same & (sub < lane)).astype(i32), axis=0, keepdims=True)
    rank_s = jnp.broadcast_to(rank_l, (TILE, SLOTS)).T
    later_s = jnp.broadcast_to(later_l, (TILE, SLOTS)).T
    chosen = rank_s == lane

    def pick(values):
        return jnp.sum(jnp.where(chosen, values, 0), axis=0, keepdims=True)

    upto = jnp.sum((key_s <= lane).astype(i32), axis=0, keepdims=True)
    count = jnp.sum((key_s == lane).astype(i32), axis=0, keepdims=True)
    meta_v[0:1, :] = pick(sub)
    meta_v[1:2, :] = pick(row_s)
    meta_v[2:3, :] = pick((later_s > 0).astype(i32))
    meta_v[3:4, :] = jnp.where(count > 0, upto - 1, LIVE)
    meta_v[4:8, :] = jnp.zeros((4, TILE), i32)
    r_v[LIVE] = jnp.zeros((WIDE_M, TILE), bf16)
    racc[...] = jnp.zeros((WIDE_M, TILE), f32)

    def spread_ids(side, part):
        table = jnp.broadcast_to(ids_v[side, part, 0:1, :], (TILE, TILE)).T
        first, count, row = ((FINE - HALO, HALO, 0), (0, FINE, HALO), (0, HALO, HALO + FINE))[part]
        ext_id[side, pl.ds(row * P_TILES, count * P_TILES), :] = table[first * P_TILES : (first + count) * P_TILES]

    def id_mask(side, index, c):
        return (ext_id[side, pl.ds(index, 1), :] == jnp.float32(c)).astype(f32).astype(bf16)

    @pl.loop(0, FINE)
    def _(i):
        first = ext[1, HALO + i, 0].T
        second = ext[1, HALO + i, 1].T
        for c in range(COARSE):
            own_t[i, c * TILE : (c + 1) * TILE, :] = first * id_mask(1, (HALO + i) * P_TILES, c) + second * id_mask(
                1, (HALO + i) * P_TILES + 1, c
            )

    meta_copy = pltpu.make_async_copy(meta_v, meta_s, meta_sem)
    meta_copy.start()
    meta_copy.wait()
    for load in loads:
        load.wait()

    @pl.loop(0, LIVE, unroll=8)
    def _(k):
        tile = a_v[jnp.clip(meta_s[0, k], 0, LIVE - 1)]
        left = own_t[jnp.clip(meta_s[1, k], 0, FINE - 1)]
        keep = meta_s[2, k].astype(f32)
        total = racc[...] * keep + jnp.dot(left, tile, preferred_element_type=f32)
        racc[...] = total
        r_v[k] = total.astype(bf16)

    def chunk_product(side, row, slot, rows=HALO):
        for l in range(rows):
            index = (row + l) * P_TILES
            first = ext[side, row + l, 0]
            second = ext[side, row + l, 1]
            for c in range(COARSE):
                phat[slot, l * TILE : (l + 1) * TILE, c * TILE : (c + 1) * TILE] = first * id_mask(
                    side, index, c
                ) + second * id_mask(side, index + 1, c)
        base = side * SPAN + row
        left = jnp.concatenate([r_v[jnp.clip(meta_s[3, base + l], 0, LIVE)] for l in range(rows)], axis=1)
        return jnp.dot(left, phat[slot, : rows * TILE, :], preferred_element_type=f32)

    def put(code, value):
        for c1 in range(COARSE):
            for c2 in range(COARSE):
                out_ref[c1, 0, code * COARSE + c2] = value[
                    c1 * TILE : (c1 + 1) * TILE, c2 * TILE : (c2 + 1) * TILE
                ].astype(bf16)

    acc[1] = chunk_product(1, HALO, 0)

    @pl.loop(1, FINE // HALO - 1)
    def _(q):
        acc[1] += chunk_product(1, HALO + q * HALO, 0)

    put(4, acc[1] + chunk_product(1, FINE, 1))

    for step in (0, 1):
        for d in (0, 1):
            side = 0 if d == 1 else 2

            @pl.when(has_side[side])
            def _():
                if step == 0:
                    to_wide_id(d).wait_recv()
                to_wide(d, step).wait_recv()

                @pl.when(has_row[step])
                def _():
                    to_rows_id(step, side).start()
                    to_rows(step, side).start()

                if step == 0:
                    spread_ids(side, 1)

        for d in (0, 1):
            side = 0 if d == 1 else 2
            value = chunk_product(side, HALO + PIECES[step][0], d)
            if step == 0:
                acc[side] = value
            else:
                acc[side] += value

    for d in (0, 1):

        @pl.when(has_row[1 - d])
        def _():
            to_rows(d, 1).wait_recv()
            to_rows_id(d, 1).wait_recv()
            spread_ids(1, 0 if d == 1 else 2)

        step = 0 if d == 1 else 2
        put(step * 3 + 1, chunk_product(1, 0 if d == 1 else HALO + FINE, d))

    for d in (0, 1):
        side = 0 if d == 1 else 2

        @pl.when(has_side[side])
        def _():
            to_wide(d, 2).wait_recv()

        acc[side] += chunk_product(side, HALO + PIECES[2][0], d)

    for d in (0, 1):
        for side in (0, 2):

            @pl.when(has_row[1 - d] & has_side[side])
            def _():
                to_rows(d, side).wait_recv()
                to_rows_id(d, side).wait_recv()
                spread_ids(side, 0 if d == 1 else 2)

            step = 0 if d == 1 else 2
            put(step * 3 + side, chunk_product(side, 0 if d == 1 else HALO + FINE, side // 2))

    for d in (0, 1):
        side = 0 if d == 1 else 2

        @pl.when(has_side[side])
        def _():
            to_wide(d, 3).wait_recv()

        acc[side] += chunk_product(side, HALO + PIECES[3][0], d, PIECES[3][1])

    for d in (0, 1):
        side = 0 if d == 1 else 2

        @pl.when(has_side[side])
        def _():
            to_wide(d, 4).wait_recv()

        put(3 + side, acc[side] + chunk_product(side, HALO + PIECES[4][0], d, PIECES[4][1]))

    for d in (0, 1):

        @pl.when(has_wide[d])
        def _():
            to_wide_id(d).wait_send()
            for piece in range(len(PIECES)):
                to_wide(d, piece).wait_send()

        @pl.when(has_row[d])
        def _():
            to_rows(d, 1).wait_send()
            to_rows_id(d, 1).wait_send()

        for side in (0, 2):

            @pl.when(has_row[d] & has_side[side])
            def _():
                to_rows(d, side).wait_send()
                to_rows_id(d, side).wait_send()


def body(matrix_tiles, row_pointers, column_blocks, prolongator_tiles, aggregate_ids):
    n_rows, n_wide = lax.axis_size("rows"), lax.axis_size("wide")
    bf16, f32, i32 = jnp.bfloat16, jnp.float32, jnp.int32
    dma = pltpu.SemaphoreType.DMA
    smem = pl.BlockSpec(memory_space=pltpu.SMEM)
    anywhere = pl.BlockSpec(memory_space=pltpu.HBM)
    vmem = pl.BlockSpec(memory_space=pltpu.VMEM)
    return pl.pallas_call(
        functools.partial(kernel, n_rows, n_wide),
        out_shape=pltpu.VMEM((COARSE, 1, 9 * COARSE, TILE, TILE), bf16),
        in_specs=[smem, smem, vmem, anywhere, anywhere],
        out_specs=vmem,
        scratch_shapes=[
            pltpu.VMEM((LIVE, TILE, TILE), bf16),
            pltpu.VMEM((3, SPAN, P_TILES, TILE, TILE), bf16),
            pltpu.VMEM((3, SPAN * P_TILES, TILE), f32),
            pltpu.VMEM((3, 3, 8, TILE), f32),
            pltpu.VMEM((FINE, WIDE_M, TILE), bf16),
            pltpu.VMEM((LIVE + 1, WIDE_M, TILE), bf16),
            pltpu.VMEM((2, HALO * TILE, WIDE_M), bf16),
            pltpu.VMEM((3, WIDE_M, WIDE_M), f32),
            pltpu.VMEM((WIDE_M, TILE), f32),
            pltpu.VMEM((8, TILE), i32),
            pltpu.SMEM((8, TILE), i32),
            dma((5,)),
            dma,
            dma((2, len(PIECES))),
            dma((2, len(PIECES))),
            dma((2,)),
            dma((2,)),
            dma((2, 3)),
            dma((2, 3)),
            dma((2, 3)),
            dma((2, 3)),
        ],
        compiler_params=pltpu.CompilerParams(
            collective_id=0, has_side_effects=True, vmem_limit_bytes=57344 * 1024
        ),
        name="galerkin",
    )(
        row_pointers.reshape(FINE + 1),
        aggregate_ids.transpose(1, 2, 0).reshape(P_TILES, FINE),
        column_blocks.reshape(1, SLOTS),
        matrix_tiles,
        prolongator_tiles,
    )


def solution(mesh):
    placed = (
        P("rows", "wide", None, None),
        P("rows", "wide"),
        P("rows", "wide"),
        P("rows", "wide", None, None, None),
        P("rows", "wide", None),
    )
    return jax.shard_map(
        body,
        mesh=mesh,
        in_specs=placed,
        out_specs=P("rows", "wide", None, None, None),
        check_vma=False,
    )
```
